128 devices in a mesh: group: 32 (over x, z, core), tensor: 4 (over y).
Axes of the slice: x: 4, y: 4, z: 4, core: 2. Of those that a mesh axis runs over, the one named last changes fastest.
Arguments:
- queries: bfloat16 [4096, 4096], P('group', 'tensor'), may hold values from -120 to 120
- keys: bfloat16 [4096, 512], P('group', 'tensor'), may hold values from -6 to 6
- values: bfloat16 [4096, 512], P('group', 'tensor'), may hold values from -6 to 6
- document_index: int32 [32, 128], P('group'), may hold values from 0 to 7, never falling along the last dimension, each value on 1 to 64 neighbouring positions
- out_proj: bfloat16 [4096, 4096], P('tensor', 'group'), may hold values from -0.25 to 0.25
- residual_in: bfloat16 [4096, 4096], P(('group', 'tensor')), may hold values from -60 to 60
- norm_gain: float32 [4096], replicated, may hold values from 0.1 to 1.9
- expert_ids: int32 [4096, 8], P(('group', 'tensor')), may hold values from 0 to 127, all different within a row; in each aligned block of 32 rows (0 to 31, 32 to 63, ...) at most 4 rows name the same one
- gate_weights: float32 [4096, 8], P(('group', 'tensor')), may hold values from 0.05 to 0.45
- w_gate_up: bfloat16 [128, 4096, 1536], P(('group', 'tensor')), may hold values from -0.09375 to 0.09375
- w_down: bfloat16 [128, 768, 4096], P(('group', 'tensor')), may hold values from -0.21875 to 0.21875
Outputs:
- layer_out: bfloat16 [4096, 4096], P(('group', 'tensor'))
The draws below stay inside these ranges and needn't reach their ends.
Inputs may be any that keep to these rules, and one draw needn't show every extreme that they name: `document_index`: ids never fall along a group's tokens; equal ids mark one document. `expert_ids`: a token names 8 different experts; among the 32 tokens of one device (aligned blocks of rows) no expert is named more than 4 times, a bound that some block reaches.
All inputs are finite; a program needn't handle non-finite values.
Results may differ from the reference program's by a relative error of at most 0.0045.
Values may be sent and summed in bfloat16 or wider, within the bound.
No kernel may reach another device: no remote copies, remote signals or barrier semaphores. Data moves between devices by JAX's collectives and lax.ppermute only.
A program may use at most 128 MiB of HBM per device.

```python
import math
import jax
import jax.numpy as jnp
import numpy as np
from jax import lax

D = 4096
QUERY_HEADS = 32
KEY_VALUE_HEADS = 4
HEAD_SIZE = 128
FF = 768
TOPK = 8
TOK_DEV = 32
GROUP_TOKENS = 128
TOTAL_TOKENS = 4096
EXPERTS = 128
CAP = 4
DOCS = 8
N_GROUP = 32


def draw_queries(key, part):
    final_output = jnp.clip(jax.random.normal(jax.random.fold_in(key, 1), (TOTAL_TOKENS, QUERY_HEADS * HEAD_SIZE), jnp.float32), -6.0, 6.0)
    return final_output.astype(jnp.bfloat16)


def draw_keys(key, part):
    final_output = jnp.clip(jax.random.normal(jax.random.fold_in(key, 2), (TOTAL_TOKENS, KEY_VALUE_HEADS * HEAD_SIZE), jnp.float32), -6.0, 6.0)
    return final_output.astype(jnp.bfloat16)


def draw_residual_in(key, part):
    row_scale = jnp.exp(jax.random.uniform(jax.random.fold_in(key, 11), (TOTAL_TOKENS, 1), jnp.float32, jnp.log(0.3), jnp.log(3.0)))
    column_scale = jnp.exp(jax.random.uniform(jax.random.fold_in(key, 12), (1, D), jnp.float32, jnp.log(0.3), jnp.log(3.0)))
    drawn_result = jnp.clip(jax.random.normal(jax.random.fold_in(key, 13), (TOTAL_TOKENS, D), jnp.float32), -6.0, 6.0)
    final_output = drawn_result * row_scale * column_scale
    return final_output.astype(jnp.bfloat16)


def block_scale(own_key, extent, split, low, largest):
    loudness = 1.0
    for dim, parts in split:
        draws = jax.random.uniform(jax.random.fold_in(jax.random.fold_in(own_key, 6), dim), (parts,), jnp.float32, low / len(split), largest / len(split))
        loudness = loudness * jnp.repeat(jnp.exp(draws), extent[dim] // parts).reshape((-1,) + (1,) * (len(extent) - 1 - dim))
    return loudness


def length_profile(number_of, total, limit, skew):
    portions = [(1 << 20) // math.isqrt(grade ** skew) + 1 for grade in range(2, number_of + 1)]
    surplus, given = total - limit - (number_of - 1), [1] * (number_of - 1)
    while surplus > 0:
        movable = [i for i in range(number_of - 1) if given[i] < limit]
        mass, remaining = sum([portions[i] for i in movable]), surplus
        for i in movable:
            more = min(limit - given[i], max(1, remaining * portions[i] // mass), surplus)
            given[i] = given[i] + more
            surplus = surplus - more
    return np.array([limit] + given)


def ragged_sizes(rng, number_of, total, bound, lean):
    if number_of == 2:
        one = jax.random.randint(rng, (), max(1, total - bound), min(bound, total - 1) + 1)
        return jnp.stack([one, total - one])
    sizes = jnp.asarray(length_profile(number_of, total, bound, lean), jnp.int32)
    couples = (number_of - 1) // 2
    donor, receiver = sizes[1:1 + 2 * couples:2], sizes[2:2 + 2 * couples:2]
    slack = jnp.minimum(donor - 1, bound - receiver)
    passed = jax.random.randint(jax.random.fold_in(rng, 1), (couples,), 0, 1 << 20) % (slack + 1)
    sizes = sizes.at[1:1 + 2 * couples:2].set(donor - passed).at[2:2 + 2 * couples:2].set(receiver + passed)
    return sizes[jax.random.permutation(jax.random.fold_in(rng, 2), number_of)]


def shared_out(own_key, own, number, rows, number_of, top, limit, slope):
    sequence = jax.random.permutation(own_key, number_of)
    packed, usual = shares(number_of, rows * top, limit, slope, True), shares(number_of, rows * top, limit, slope, False)
    places = jnp.arange(number_of)

    def named(tallies, offset_by):
        used = int((tallies > 0).sum())
        fixed = max(1, used // 4)
        passed = fixed + (places - fixed + offset_by * (used - fixed)) % max(1, number_of - fixed)
        return jnp.zeros((number_of,), jnp.int32).at[sequence[jnp.where(places < fixed, places, passed)]].set(jnp.asarray(tallies, jnp.int32))

    tallies = jnp.where(number % 4 == 0, named(packed, number // 4), named(usual, number - number // 4 - 1))
    mixed = jax.random.permutation(jax.random.fold_in(own, 3), number_of)
    donor, receiver = mixed[0:number_of // 2 * 2:2], mixed[1:number_of // 2 * 2:2]
    room = jnp.minimum(tallies[donor] - 1, limit - tallies[receiver]) // 2
    room = jnp.where((donor == sequence[0]) | (receiver == sequence[0]) | (tallies[receiver] == 0), 0, jnp.maximum(room, 0))
    passed = jax.random.randint(jax.random.fold_in(own, 4), (number_of // 2,), 0, 1 << 20) % (room + 1)
    tallies = tallies.at[donor].add(-passed).at[receiver].add(passed)
    items = jnp.searchsorted(jnp.cumsum(tallies), jnp.arange(rows * top), side="right").astype(jnp.int32)
    table = items.reshape(top, rows).T
    table = table[jax.random.permutation(jax.random.fold_in(own, 1), rows)]
    offset_by = jax.random.randint(jax.random.fold_in(own, 2), (rows, 1), 0, top)
    return jnp.take_along_axis(table, (jnp.arange(top)[None, :] + offset_by) % top, axis=1)


def shares(amount, total, limit, lean, full):
    portions = [(1 << 20) // math.isqrt(grade ** lean) + 1 for grade in range(1, amount + 1)]
    largest = limit if full else min(limit, max(-(-total // amount), total * portions[0] // sum(portions)))
    least = 1 if total - largest >= amount - 1 else 0
    counts, rest = [largest] + [least] * (amount - 1), total - largest - least * (amount - 1)
    while rest > 0:
        candidates = [i for i in range(1, amount) if counts[i] < largest] or [i for i in range(1, amount) if counts[i] < limit]
        whole, budget = sum([portions[i] for i in candidates]), rest
        for i in candidates:
            extra = min(limit - counts[i], max(1, budget * portions[i] // whole), rest)
            counts[i] = counts[i] + extra
            rest = rest - extra
    return np.array(counts)


def scatter_about(rng, shape, width, reach, shards=(), kind=jnp.bfloat16):
    entries = width * jax.random.normal(rng, shape, jnp.float32)
    if shards:
        entries = entries * block_scale(rng, shape, shards, -0.22, 0.18)
    return jnp.clip(entries, -reach, reach).astype(kind)


def setup_inputs(seed: int = 0) -> dict:
    streams_of = jax.random.split(jax.random.key(seed), 12)
    queries = draw_queries(jax.random.fold_in(streams_of[11], 71), 0)
    keys = draw_keys(jax.random.fold_in(streams_of[11], 71), 0)
    values = scatter_about(streams_of[2], (TOTAL_TOKENS, KEY_VALUE_HEADS * HEAD_SIZE), 1.0, 6.0, ((0, 32), (1, 4)))
    document_index = jax.vmap(lambda own: jnp.searchsorted(jnp.cumsum(ragged_sizes(own, DOCS, GROUP_TOKENS, GROUP_TOKENS // 2, 2)), jnp.arange(GROUP_TOKENS), side="right"))(jax.random.split(streams_of[3], N_GROUP)).reshape((N_GROUP, GROUP_TOKENS)).astype(jnp.int32)
    out_proj = scatter_about(streams_of[4], (QUERY_HEADS * HEAD_SIZE, D), (QUERY_HEADS * HEAD_SIZE // 8) ** -0.5, 0.25, ((0, 4), (1, 32)))
    residual_in = draw_residual_in(jax.random.fold_in(streams_of[11], 71), 0)
    norm_gain = jnp.clip(1.0 + 0.18 * jax.random.normal(streams_of[6], (D,), jnp.float32), 0.1, 1.9)
    expert_ids_keys = jax.random.split(jax.random.fold_in(streams_of[7], 1), TOTAL_TOKENS // TOK_DEV)
    expert_ids_turns = jax.random.permutation(jax.random.fold_in(streams_of[7], 3), TOTAL_TOKENS // TOK_DEV)
    expert_ids = jax.vmap(lambda own, number: shared_out(jax.random.fold_in(streams_of[7], 2), own, number, TOK_DEV, EXPERTS, TOPK, CAP, 2))(expert_ids_keys, expert_ids_turns).reshape((TOTAL_TOKENS, TOPK))
    gate_weights = jnp.clip(0.05 + 0.39999999 * jax.random.uniform(streams_of[8], (TOTAL_TOKENS, TOPK), jnp.float32) ** block_scale(streams_of[8], (TOTAL_TOKENS, TOPK), ((0, 128),), -0.2, 0.2), 0.05, 0.45)
    w_gate_up = scatter_about(streams_of[9], (EXPERTS, D, 2 * FF), D ** -0.5, 0.09375, ((0, 128),))
    w_down = scatter_about(streams_of[10], (EXPERTS, FF, D), FF ** -0.5, 0.21875, ((0, 128),))
    return dict(queries=queries, keys=keys, values=values, document_index=document_index, out_proj=out_proj, residual_in=residual_in, norm_gain=norm_gain, expert_ids=expert_ids, gate_weights=gate_weights, w_gate_up=w_gate_up, w_down=w_down)


def attend(query_matrix, key_matrix, value_matrix, doc_row):
    token_group = query_matrix.shape[0]
    query_head_split = query_matrix.reshape(token_group, KEY_VALUE_HEADS, QUERY_HEADS // KEY_VALUE_HEADS, HEAD_SIZE).astype(jnp.float32)
    key_head_split = key_matrix.reshape(token_group, KEY_VALUE_HEADS, HEAD_SIZE).astype(jnp.float32)
    value_head_split = value_matrix.reshape(token_group, KEY_VALUE_HEADS, HEAD_SIZE).astype(jnp.float32)
    scores = jnp.einsum('qgrd,kgd->grqk', query_head_split, key_head_split) * (1.0 / HEAD_SIZE ** 0.5)
    positions = jnp.arange(token_group, dtype=jnp.int32)
    visible = (positions[:, None] >= positions[None, :]) & (doc_row[:, None] == doc_row[None, :])
    scores = jnp.where(visible, scores, -jnp.inf)
    row_max = lax.optimization_barrier(jnp.max(scores, axis=-1, keepdims=True))
    exponent = jnp.where(visible, jnp.exp(scores - row_max), 0.0)
    weights = (exponent / lax.optimization_barrier(jnp.sum(exponent, axis=-1, keepdims=True))).astype(jnp.bfloat16)
    head_out = jnp.einsum('grqk,kgd->qgrd', weights.astype(jnp.float32), value_head_split)
    return head_out.astype(jnp.bfloat16).reshape(token_group, QUERY_HEADS * HEAD_SIZE)

def reference(queries, keys, values, document_index, out_proj, residual_in, norm_gain, expert_ids, gate_weights, w_gate_up, w_down):
    head_grouped = (queries.reshape(N_GROUP, GROUP_TOKENS, QUERY_HEADS * HEAD_SIZE), keys.reshape(N_GROUP, GROUP_TOKENS, KEY_VALUE_HEADS * HEAD_SIZE), values.reshape(N_GROUP, GROUP_TOKENS, KEY_VALUE_HEADS * HEAD_SIZE), document_index)

    def per_group(inputs):
        return attend(inputs[0], inputs[1], inputs[2], inputs[3])
    head_out = lax.map(per_group, head_grouped).reshape(TOTAL_TOKENS, QUERY_HEADS * HEAD_SIZE)
    hidden = residual_in.astype(jnp.float32) + jnp.dot(head_out, out_proj, preferred_element_type=jnp.float32)
    mean_square = lax.optimization_barrier(jnp.mean(hidden * hidden, axis=-1, keepdims=True))
    normed = (hidden * lax.rsqrt(mean_square + 1e-06) * norm_gain.astype(jnp.float32)).astype(jnp.bfloat16)
    flat_ids = expert_ids.reshape(-1).astype(jnp.int32)
    flat_gate = gate_weights.reshape(-1).astype(jnp.float32)
    token_index = (jnp.arange(TOTAL_TOKENS * TOPK, dtype=jnp.int32) // TOPK).astype(jnp.int32)
    slot_rows = EXPERTS * CAP

    def per_expert(moe_total, inputs):
        expert, gate_up, down_rows = inputs
        chosen = flat_ids == expert
        position = jnp.cumsum(chosen.astype(jnp.int32)) - 1
        position = jnp.where(chosen, position, slot_rows).astype(jnp.int32)
        sources = jnp.zeros((slot_rows,), jnp.int32).at[position].set(token_index, mode='drop')
        weight = jnp.zeros((slot_rows,), jnp.float32).at[position].set(flat_gate, mode='drop')
        gathered_rows = normed[sources]
        projected = jnp.dot(gathered_rows, gate_up, preferred_element_type=jnp.float32)
        activated = (jax.nn.silu(projected[:, :FF]) * projected[:, FF:]).astype(jnp.bfloat16)
        expert_out = jnp.dot(activated, down_rows, preferred_element_type=jnp.float32).astype(jnp.bfloat16)
        moe_total = moe_total.at[sources].add(expert_out.astype(jnp.float32) * weight[:, None])
        return (moe_total, None)
    moe_total, _ = lax.scan(per_expert, jnp.zeros((TOTAL_TOKENS, D), jnp.float32), (jnp.arange(EXPERTS, dtype=jnp.int32), w_gate_up, w_down))
    return (hidden + moe_total).astype(jnp.bfloat16)
```

```python
import jax
import jax.numpy as jnp
from jax import lax
from jax.experimental import pallas as pl
from jax.experimental.pallas import tpu as pltpu
from jax.sharding import Mesh, PartitionSpec as P

HEAD_SIZE = 128
SLOTS = 4
VMEM = pltpu.VMEM
SMEM = pltpu.SMEM
F32 = jnp.float32
BF16 = jnp.bfloat16


def dot(a, b, dims=((1,), (0,))):
    return lax.dot_general(a, b, (dims, ((), ())), preferred_element_type=F32)


def vspec():
    return pl.BlockSpec(memory_space=VMEM)


def sspec():
    return pl.BlockSpec(memory_space=SMEM)


def ring(value, axis, shift, length):
    return lax.ppermute(value, axis, [(i, (i - shift) % length) for i in range(length)])


def attention_body(q_ref, k_ref, v_ref, doc_ref, out_ref):
    tokens = q_ref.shape[0]
    doc = jnp.broadcast_to(doc_ref[...].astype(F32), (tokens, tokens))
    row = lax.broadcasted_iota(jnp.int32, (tokens, tokens), 0)
    col = lax.broadcasted_iota(jnp.int32, (tokens, tokens), 1)
    visible = (row >= col) & (doc == doc.T)
    key = k_ref[...]
    value = v_ref[...]
    for h in range(q_ref.shape[1] // HEAD_SIZE):
        cols = slice(h * HEAD_SIZE, (h + 1) * HEAD_SIZE)
        scores = dot(q_ref[:, cols], key, ((1,), (1,))) * (1.0 / HEAD_SIZE**0.5)
        scores = jnp.where(visible, scores, -jnp.inf)
        top = jnp.max(scores, axis=-1, keepdims=True)
        exponent = jnp.where(visible, jnp.exp(scores - top), 0.0)
        probs = (exponent / jnp.sum(exponent, axis=-1, keepdims=True)).astype(BF16)
        out_ref[:, cols] = dot(probs, value).astype(BF16)


def project_body(place_ref, h0, h1, h2, h3, own_ref, other_ref, out_ref):
    x, z, c = place_ref[0], place_ref[1], place_ref[2]
    tok = h0.shape[0] // 4
    for w_ref, core in ((own_ref, c), (other_ref, 1 - c)):
        weight = w_ref[...]
        for s, h_ref in enumerate((h0, h1, h2, h3)):
            part = dot(h_ref[...], weight).astype(BF16)
            dest = lax.rem(x + s, 4)
            for t in range(4):
                at = pl.multiple_of((lax.rem(z + t, 4) * 2 + core) * 128, 128)
                for y in range(4):
                    out_ref[dest * 4 + y, :, pl.ds(at, 128)] = part[
                        y * tok : (y + 1) * tok, t * 128 : (t + 1) * 128
                    ]


def norm_body(parts_ref, residual_ref, gain_ref, hidden_ref, normed_ref):
    width = parts_ref.shape[2]
    tok, model = residual_ref.shape
    square = jnp.zeros((tok, 1), F32)
    for b in range(4):
        cols = slice(b * width, (b + 1) * width)
        total = parts_ref[4 * b].astype(F32)
        for y in range(1, 4):
            total = total + parts_ref[4 * b + y].astype(F32)
        total = residual_ref[:, cols].astype(F32) + total
        hidden_ref[:, cols] = total
        square = square + jnp.sum(total * total, axis=-1, keepdims=True)
    scale = lax.rsqrt(square * (1.0 / model) + 1e-06)
    normed_ref[...] = (hidden_ref[...] * scale * gain_ref[...]).astype(BF16)


def routing(core, ids, slots):
    tokens = ids.shape[0]
    half = tokens // 2
    slot = lax.broadcasted_iota(jnp.int32, (tokens, slots), 1)
    token = lax.broadcasted_iota(jnp.int32, (tokens, slots), 0)
    chip = slot // (2 * SLOTS)
    expert = ((chip // 4) * 2 + core) * 4 + chip % 4
    named = [ids[:, j : j + 1] == expert for j in range(ids.shape[1])]
    match = named[0]
    for one in named[1:]:
        match = match | one
    r = lax.broadcasted_iota(jnp.int32, (tokens, tokens), 0)
    c = lax.broadcasted_iota(jnp.int32, (tokens, tokens), 1)
    ahead = (c < r) & ((c < half) == (r < half))
    rank = dot(ahead.astype(BF16), match.astype(BF16)).astype(jnp.int32)
    here = match & (rank == slot % SLOTS) & ((token < half) == (slot % (2 * SLOTS) < SLOTS))
    return here, named


def dispatch_body(place_ref, own_ref, other_ref, ids_ref, out_ref):
    slots = out_ref.shape[0]
    here, _ = routing(place_ref[2], ids_ref[...], slots)
    table = here.astype(BF16)
    tokens = jnp.concatenate([own_ref[...], other_ref[...]], axis=0)
    out_ref[...] = dot(table, tokens, ((0,), (0,))).astype(BF16)


def combine_body(place_ref, results_ref, ids_ref, gates_ref, own_ref, other_ref):
    slots = results_ref.shape[0]
    here, named = routing(place_ref[2], ids_ref[...], slots)
    gates = gates_ref[...]
    weight = jnp.zeros(here.shape, F32)
    for j, one in enumerate(named):
        weight = weight + jnp.where(one, gates[:, j : j + 1], 0.0)
    weight = jnp.where(here, weight, 0.0)
    high = weight.astype(BF16)
    low = (weight - high.astype(F32)).astype(BF16)
    results = results_ref[...]
    total = dot(high, results) + dot(low, results)
    half = total.shape[0] // 2
    own_ref[...] = total[:half]
    other_ref[...] = total[half:]


def finish_body(hidden_ref, own_ref, other_ref, out_ref):
    out_ref[...] = (hidden_ref[...] + (own_ref[...] + other_ref[...])).astype(BF16)


def on_device(
    queries,
    keys,
    values,
    document_index,
    out_proj,
    residual_in,
    norm_gain,
    expert_ids,
    gate_weights,
    w_gate_up,
    w_down,
):
    place = jnp.stack([lax.axis_index(a) for a in ("x", "z", "c")]).astype(jnp.int32)
    tok, model = residual_in.shape
    tokens, head_cols = queries.shape
    ff = w_down.shape[1]

    pieces = [out_proj] + [ring(out_proj, "z", s, 4) for s in (1, 2, 3)]
    own_cols = jnp.concatenate(pieces, axis=1)
    other_cols = ring(own_cols, "c", 1, 2)

    route = jnp.concatenate([expert_ids.astype(F32), gate_weights], axis=1)
    route = jnp.concatenate([route, ring(route, "c", 1, 2)], axis=0)
    ids = route[:, :8].astype(jnp.int32)
    gates = route[:, 8:]

    heads = pl.pallas_call(
        attention_body,
        out_shape=jax.ShapeDtypeStruct((tokens, head_cols), BF16),
        in_specs=[vspec()] * 4,
        out_specs=vspec(),
        name="attention",
    )(queries, keys, values, document_index)
    all_heads = [heads] + [ring(heads, "x", s, 4) for s in (1, 2, 3)]

    parts = pl.pallas_call(
        project_body,
        out_shape=jax.ShapeDtypeStruct((16, tok, model // 4), BF16),
        in_specs=[sspec()] + [vspec()] * 6,
        out_specs=vspec(),
        name="project",
    )(place, *all_heads, own_cols, other_cols)
    parts = lax.all_to_all(parts, ("x", "y"), 0, 0, tiled=True)

    hidden, normed = pl.pallas_call(
        norm_body,
        out_shape=(
            jax.ShapeDtypeStruct((tok, model), F32),
            jax.ShapeDtypeStruct((tok, model), BF16),
        ),
        in_specs=[vspec()] * 3,
        out_specs=(vspec(), vspec()),
        name="norm",
    )(parts, residual_in, norm_gain.reshape(1, model))

    slots = 64 * 2 * SLOTS
    outgoing = pl.pallas_call(
        dispatch_body,
        out_shape=jax.ShapeDtypeStruct((slots, model), BF16),
        in_specs=[sspec()] + [vspec()] * 3,
        out_specs=vspec(),
        name="dispatch",
    )(place, normed, ring(normed, "c", 1, 2), ids)
    rows = lax.all_to_all(
        outgoing.reshape(64, 2 * SLOTS, model), ("x", "z", "y"), 0, 0, tiled=True
    ).reshape(slots, model)

    projected = dot(rows, w_gate_up[0])
    activated = (jax.nn.silu(projected[:, :ff]) * projected[:, ff:]).astype(BF16)
    expert_out = dot(activated, w_down[0]).astype(BF16)

    results = lax.all_to_all(
        expert_out.reshape(64, 2 * SLOTS, model), ("x", "z", "y"), 0, 0, tiled=True
    ).reshape(slots, model)
    own, other = pl.pallas_call(
        combine_body,
        out_shape=(jax.ShapeDtypeStruct((tok, model), F32),) * 2,
        in_specs=[sspec()] + [vspec()] * 3,
        out_specs=(vspec(), vspec()),
        name="combine",
    )(place, results, ids, gates)
    return pl.pallas_call(
        finish_body,
        out_shape=jax.ShapeDtypeStruct((tok, model), BF16),
        in_specs=[vspec()] * 3,
        out_specs=vspec(),
        name="finish",
    )(hidden, own, ring(other, "c", 1, 2))


def solution(mesh):
    fine = Mesh(mesh.devices.reshape(4, 4, 2, 4), ("x", "z", "c", "y"))
    group = ("x", "z", "c")
    every = group + ("y",)
    in_specs = (
        P(group, "y"),
        P(group, "y"),
        P(group, "y"),
        P(group, None),
        P("y", group),
        P(every, None),
        P(),
        P(every, None),
        P(every, None),
        P(every, None, None),
        P(every, None, None),
    )
    return jax.shard_map(
        on_device, mesh=fine, in_specs=in_specs, out_specs=P(every, None), check_vma=False
    )
```

```python
import jax
import jax.numpy as jnp
from jax import lax
from jax.experimental import pallas as pl
from jax.experimental.pallas import tpu as pltpu
from jax.sharding import Mesh, PartitionSpec as P

HEAD_SIZE = 128
SLOTS = 4
VMEM = pltpu.VMEM
SMEM = pltpu.SMEM
F32 = jnp.float32
BF16 = jnp.bfloat16


def dot(a, b, dims=((1,), (0,))):
    return lax.dot_general(a, b, (dims, ((), ())), preferred_element_type=F32)


def vspec():
    return pl.BlockSpec(memory_space=VMEM)


def sspec():
    return pl.BlockSpec(memory_space=SMEM)


def call(body, outs, *args, flops=0, limit=8, out=True, hbm=(), scratch=()):
    specs, placed = [], []
    for a in args:
        if a.dtype == jnp.int32 and a.ndim == 1:
            specs.append(sspec())
            placed.append(a)
        elif any(a is h for h in hbm):
            specs.append(pl.BlockSpec(memory_space=pl.ANY))
            placed.append(pltpu.with_memory_space_constraint(a, pltpu.HBM))
        else:
            specs.append(vspec())
            placed.append(pltpu.with_memory_space_constraint(a, VMEM))
    single = not isinstance(outs, list)
    shapes = [outs] if single else outs
    out_shape = [VMEM(o.shape, o.dtype) for o in shapes] if out else shapes
    result = pl.pallas_call(
        body,
        out_shape=out_shape,
        in_specs=specs,
        out_specs=[vspec()] * len(shapes),
        scratch_shapes=list(scratch),
        compiler_params=pltpu.CompilerParams(vmem_limit_bytes=limit * 2**20),
        cost_estimate=pl.CostEstimate(flops=flops, bytes_accessed=0, transcendentals=0),
    )(*placed)
    return result[0] if single else result


def shape(dims, dtype):
    return jax.ShapeDtypeStruct(dims, dtype)


def ring(value, axis, shift, length):
    return lax.ppermute(value, axis, [(i, (i - shift) % length) for i in range(length)])


CHUNKS = 4


def attention_body(
    q_hbm, k_hbm, v_hbm, doc_hbm, up_hbm, out_ref, up_ref, q_ref, k_ref, v_ref, doc_ref, sems, load
):
    pairs = ((doc_hbm, doc_ref), (k_hbm, k_ref), (v_hbm, v_ref), (q_hbm, q_ref))
    copies = [pltpu.make_async_copy(h, v, sems.at[i]) for i, (h, v) in enumerate(pairs)]
    for copy in copies:
        copy.start()
    rows = up_ref.shape[0]
    wide = pltpu.make_async_copy(up_hbm.at[0, pl.ds(0, rows), :], up_ref, load)
    wide.start()
    for copy in copies:
        copy.wait()
    tokens = q_ref.shape[0]
    doc = jnp.broadcast_to(doc_ref[...].astype(F32), (tokens, tokens))
    row = lax.broadcasted_iota(jnp.int32, (tokens, tokens), 0)
    col = lax.broadcasted_iota(jnp.int32, (tokens, tokens), 1)
    visible = (row >= col) & (doc == doc.T)
    key = k_ref[...]
    value = v_ref[...]
    for h in range(q_ref.shape[1] // HEAD_SIZE):
        cols = slice(h * HEAD_SIZE, (h + 1) * HEAD_SIZE)
        scores = dot(q_ref[:, cols], key, ((1,), (1,))) * (1.0 / HEAD_SIZE**0.5)
        scores = jnp.where(visible, scores, -jnp.inf)
        top = jnp.max(scores, axis=-1, keepdims=True)
        exponent = jnp.where(visible, jnp.exp(scores - top), 0.0)
        probs = (exponent / jnp.sum(exponent, axis=-1, keepdims=True)).astype(BF16)
        out_ref[:, cols] = dot(probs, value).astype(BF16)
    wide.wait()


def join_body(a, b, c, d, out_ref):
    for i, ref in enumerate((a, b, c, d)):
        out_ref[:, i * 128 : (i + 1) * 128] = ref[...]


def project_body(own_ref, other_ref, *refs):
    z, c, y = lax.axis_index("z"), lax.axis_index("c"), lax.axis_index("y")
    pieces, outs = refs[:-4], refs[-4:]
    tok = pieces[0].shape[0] // 4
    wide = own_ref.shape[1] // 4
    own, other = own_ref[...], other_ref[...]
    for s, out_ref in enumerate(outs):
        rows = pl.ds(pl.multiple_of(lax.rem(y + s, 4) * tok, tok), tok)
        heads = jnp.concatenate([piece[rows, :] for piece in pieces], axis=0)
        for weight, core in ((own, c), (other, 1 - c)):
            part = dot(heads, weight).astype(BF16)
            for t in range(4):
                at = pl.multiple_of((lax.rem(z + t, 4) * 2 + core) * wide, wide)
                out_ref[:, pl.ds(at, wide)] = part[:, t * wide : (t + 1) * wide]


def total_body(a, b, c, d, *outs):
    tok = outs[0].shape[0]
    for i, out_ref in enumerate(outs):
        rows = slice(i * tok, (i + 1) * tok)
        total = a[rows, :].astype(F32) + b[rows, :].astype(F32)
        total = total + c[rows, :].astype(F32) + d[rows, :].astype(F32)
        out_ref[...] = total.astype(out_ref.dtype)


def norm_body(p0, p1, p2, p3, residual_ref, gain_ref, hidden_ref, normed_ref):
    x = lax.axis_index("x")
    tok, model = residual_ref.shape
    width = model // 4
    square = jnp.zeros((tok, 1), F32)
    for s, piece in enumerate((p0, p1, p2, p3)):
        cols = pl.ds(pl.multiple_of(lax.rem(x + 4 - s, 4) * width, width), width)
        total = residual_ref[:, cols].astype(F32) + piece[...].astype(F32)
        hidden_ref[:, cols] = total
        square = square + jnp.sum(total * total, axis=-1, keepdims=True)
    scale = lax.rsqrt(square * (1.0 / model) + 1e-06)
    normed_ref[...] = (hidden_ref[...] * scale * gain_ref[...]).astype(BF16)


def routing(core, ids, slots):
    tokens = ids.shape[0]
    half = tokens // 2
    slot = lax.broadcasted_iota(jnp.int32, (tokens, slots), 1)
    token = lax.broadcasted_iota(jnp.int32, (tokens, slots), 0)
    chip = slot // (2 * SLOTS)
    expert = ((chip // 4) * 2 + core) * 4 + chip % 4
    named = [ids[:, j : j + 1] == expert for j in range(ids.shape[1])]
    match = named[0]
    for one in named[1:]:
        match = match | one
    r = lax.broadcasted_iota(jnp.int32, (tokens, tokens), 0)
    c = lax.broadcasted_iota(jnp.int32, (tokens, tokens), 1)
    ahead = (c < r) & ((c < half) == (r < half))
    rank = dot(ahead.astype(BF16), match.astype(BF16)).astype(jnp.int32)
    here = match & (rank == slot % SLOTS) & ((token < half) == (slot % (2 * SLOTS) < SLOTS))
    return here, named


def expert_body(
    rows_ref, first_ref, up_hbm, down_ref, out_ref, sum_ref, second_ref, act_ref, sems
):
    tile, ff = act_ref.shape
    half = first_ref.shape[0]
    rows = half // CHUNKS
    copies = [
        pltpu.make_async_copy(
            up_hbm.at[0, pl.ds(half + i * rows, rows), :],
            second_ref.at[pl.ds(i * rows, rows), :],
            sems.at[i],
        )
        for i in range(CHUNKS)
    ]
    for copy in copies:
        copy.start()
    steps = rows_ref.shape[0] // tile

    def begin(m, carry):
        at = pl.ds(pl.multiple_of(m * tile, tile), tile)
        sum_ref[at, :] = dot(rows_ref[at, :half], first_ref[...])
        return carry

    def step(m, carry):
        at = pl.ds(pl.multiple_of(m * tile, tile), tile)
        right = rows_ref[at, half:]
        gate = sum_ref[at, :ff] + dot(right, second_ref[:, :ff])
        up = sum_ref[at, ff:] + dot(right, second_ref[:, ff:])
        act_ref[...] = (gate / (1.0 + jnp.exp(-gate)) * up).astype(BF16)
        out_ref[at, :] = dot(act_ref[...], down_ref[...]).astype(BF16)
        return carry

    lax.fori_loop(0, steps, begin, 0)
    for copy in copies:
        copy.wait()
    lax.fori_loop(0, steps, step, 0)


def pack_body(ids_ref, gates_ref, out_ref):
    top = ids_ref.shape[0]
    out_ref[:top] = ids_ref[...].astype(F32)
    out_ref[top:] = gates_ref[...]


def tables_body(own_ref, sibling_ref, table_ref, weights_ref):
    tokens, slots = table_ref.shape
    top = own_ref.shape[0] // 2
    route = jnp.concatenate([own_ref[...].T, sibling_ref[...].T], axis=0)
    ids = route[:, :top].astype(jnp.int32)
    gates = route[:, top:]
    here, named = routing(lax.axis_index("c"), ids, slots)
    weight = jnp.zeros(here.shape, F32)
    for j, one in enumerate(named):
        weight = weight + jnp.where(one, gates[:, j : j + 1], 0.0)
    weight = jnp.where(here, weight, 0.0)
    high = weight.astype(BF16)
    table_ref[...] = here.astype(BF16)
    weights_ref[:tokens] = high
    weights_ref[tokens:] = (weight - high.astype(F32)).astype(BF16)


def dispatch_body(table_ref, own_ref, other_ref, out_ref):
    tokens = jnp.concatenate([own_ref[...], other_ref[...]], axis=0)
    out_ref[...] = dot(table_ref[...], tokens, ((0,), (0,))).astype(BF16)


def combine_body(results_ref, weights_ref, hidden_ref, own_ref, other_ref):
    total = dot(weights_ref[...], results_ref[...])
    tok = hidden_ref.shape[0]
    other_ref[...] = total[tok : 2 * tok] + total[3 * tok :]
    own_ref[...] = hidden_ref[...] + (total[:tok] + total[2 * tok : 3 * tok])


def finish_body(own_ref, other_ref, out_ref):
    out_ref[...] = (own_ref[...] + other_ref[...]).astype(BF16)


def layer(
    queries,
    keys,
    values,
    document_index,
    out_proj,
    residual_in,
    norm_gain,
    expert_ids,
    gate_weights,
    w_gate_up,
    w_down,
):
    tok, model = residual_in.shape
    tokens, head_cols = queries.shape
    ff = w_down.shape[1]
    slots = 64 * 2 * SLOTS
    width = model // 4

    columns = [ring(out_proj, "z", s, 4) for s in (1, 2, 3)]
    inputs = (queries, keys, values, document_index)
    half_rows = shape((model // 2, 2 * ff), BF16)
    heads, first = call(
        attention_body, [shape((tokens, head_cols), BF16), half_rows],
        *inputs, w_gate_up, flops=10**10, hbm=(*inputs, w_gate_up),
        scratch=[VMEM(a.shape, a.dtype) for a in inputs]
        + [pltpu.SemaphoreType.DMA((4,)), pltpu.SemaphoreType.DMA(())],
    )
    near = [heads] + [ring(heads, "x", s, 4) for s in (1, 3)]
    far = [ring(heads, "x", 2, 4)]
    own_cols = call(
        join_body, shape((head_cols, model // 8), BF16),
        out_proj, *columns,
    )
    other_cols = ring(own_cols, "c", 1, 2)

    route = call(
        pack_body, shape((2 * expert_ids.shape[1], tok), F32),
        expert_ids.T, gate_weights.T,
    )
    sibling = ring(route, "c", 1, 2)
    table, weights = call(
        tables_body, [shape((2 * tok, slots), BF16), shape((4 * tok, slots), BF16)],
        route, sibling,
    )

    parts = {}
    for name, pieces in (("near", near), ("far", far)):
        outs = [shape((len(pieces) * tok, width), BF16)] * 4
        operands = (own_cols, other_cols, *pieces)
        mine, *sent = call(project_body, outs, *operands, flops=10**9)
        got = [ring(v, "y", -s, 4) for s, v in zip((1, 2, 3), sent)]
        kinds = [F32, BF16, BF16] if name == "near" else [BF16]
        sums = call(total_body, [shape((tok, width), k) for k in kinds], mine, *got)
        for s, v in zip((0, 1, 3) if name == "near" else (2,), sums):
            parts[s] = ring(v, "x", -s, 4) if s else v

    hidden, normed = call(
        norm_body, [shape((tok, model), F32), shape((tok, model), BF16)],
        *[parts[s] for s in range(4)], residual_in, norm_gain.reshape(1, model),
    )

    outgoing = call(
        dispatch_body, shape((slots, model), BF16),
        table, normed, ring(normed, "c", 1, 2),
    )
    rows = lax.all_to_all(
        outgoing.reshape(64, 2 * SLOTS, model), ("x", "z", "y"), 0, 0, tiled=True
    ).reshape(slots, model)

    expert_out = call(
        expert_body, shape((slots, model), BF16), rows, first, w_gate_up, w_down[0],
        flops=10**10, hbm=(w_gate_up,), limit=16,
        scratch=[
            VMEM((slots, 2 * ff), F32),
            VMEM(half_rows.shape, BF16),
            VMEM((256, ff), BF16),
            pltpu.SemaphoreType.DMA((CHUNKS,)),
        ],
    )
    results = lax.all_to_all(
        expert_out.reshape(64, 2 * SLOTS, model), ("x", "z", "y"), 0, 0, tiled=True
    ).reshape(slots, model)
    own, other = call(combine_body, [shape((tok, model), F32)] * 2, results, weights, hidden)
    return call(finish_body, shape((tok, model), BF16), own, ring(other, "c", 1, 2), out=False)


def solution(mesh):
    fine = Mesh(mesh.devices.reshape(4, 4, 2, 4), ("x", "z", "c", "y"))
    group = ("x", "z", "c")
    every = group + ("y",)
    in_specs = (
        P(group, "y"),
        P(group, "y"),
        P(group, "y"),
        P(group, None),
        P("y", group),
        P(every, None),
        P(),
        P(every, None),
        P(every, None),
        P(every, None, None),
        P(every, None, None),
    )
    return jax.shard_map(
        layer, mesh=fine, in_specs=in_specs, out_specs=P(every, None), check_vma=False
    )
```

```python
import jax
import jax.numpy as jnp
from jax import lax
from jax.experimental import pallas as pl
from jax.experimental.pallas import tpu as pltpu
from jax.sharding import Mesh, PartitionSpec as P

HEAD_SIZE = 128
SLOTS = 4
VMEM = pltpu.VMEM
SMEM = pltpu.SMEM
F32 = jnp.float32
BF16 = jnp.bfloat16


def dot(a, b, dims=((1,), (0,))):
    return lax.dot_general(a, b, (dims, ((), ())), preferred_element_type=F32)


def vspec():
    return pl.BlockSpec(memory_space=VMEM)


def sspec():
    return pl.BlockSpec(memory_space=SMEM)


def call(body, outs, *args, flops=0, limit=8, out=True, hbm=(), scratch=()):
    specs, placed = [], []
    for a in args:
        if a.dtype == jnp.int32 and a.ndim == 1:
            specs.append(sspec())
            placed.append(a)
        elif any(a is h for h in hbm):
            specs.append(pl.BlockSpec(memory_space=pl.ANY))
            placed.append(pltpu.with_memory_space_constraint(a, pltpu.HBM))
        else:
            specs.append(vspec())
            placed.append(pltpu.with_memory_space_constraint(a, VMEM))
    single = not isinstance(outs, list)
    shapes = [outs] if single else outs
    out_shape = [VMEM(o.shape, o.dtype) for o in shapes] if out else shapes
    result = pl.pallas_call(
        body,
        out_shape=out_shape,
        in_specs=specs,
        out_specs=[vspec()] * len(shapes),
        scratch_shapes=list(scratch),
        compiler_params=pltpu.CompilerParams(vmem_limit_bytes=limit * 2**20),
        cost_estimate=pl.CostEstimate(flops=flops, bytes_accessed=0, transcendentals=0),
    )(*placed)
    return result[0] if single else result


def shape(dims, dtype):
    return jax.ShapeDtypeStruct(dims, dtype)


def ring(value, axis, shift, length):
    return lax.ppermute(value, axis, [(i, (i - shift) % length) for i in range(length)])


def attention_body(
    q_hbm, k_hbm, v_hbm, doc_hbm, up_hbm, out_ref, up_ref, q_ref, k_ref, v_ref, doc_ref, sems, load
):
    pairs = ((doc_hbm, doc_ref), (k_hbm, k_ref), (v_hbm, v_ref), (q_hbm, q_ref))
    copies = [pltpu.make_async_copy(h, v, sems.at[i]) for i, (h, v) in enumerate(pairs)]
    for copy in copies:
        copy.start()
    rows = up_ref.shape[0]
    wide = pltpu.make_async_copy(up_hbm.at[0, pl.ds(0, rows), :], up_ref, load)
    wide.start()
    for copy in copies:
        copy.wait()
    tokens = q_ref.shape[0]
    doc = jnp.broadcast_to(doc_ref[...].astype(F32), (tokens, tokens))
    row = lax.broadcasted_iota(jnp.int32, (tokens, tokens), 0)
    col = lax.broadcasted_iota(jnp.int32, (tokens, tokens), 1)
    visible = (row >= col) & (doc == doc.T)
    key = k_ref[...]
    value = v_ref[...]
    for h in range(q_ref.shape[1] // HEAD_SIZE):
        cols = slice(h * HEAD_SIZE, (h + 1) * HEAD_SIZE)
        scores = dot(q_ref[:, cols], key, ((1,), (1,))) * (1.0 / HEAD_SIZE**0.5)
        scores = jnp.where(visible, scores, -jnp.inf)
        top = jnp.max(scores, axis=-1, keepdims=True)
        exponent = jnp.where(visible, jnp.exp(scores - top), 0.0)
        probs = (exponent / jnp.sum(exponent, axis=-1, keepdims=True)).astype(BF16)
        out_ref[:, cols] = dot(probs, value).astype(BF16)
    wide.wait()


def join_body(a, b, c, d, out_ref):
    for i, ref in enumerate((a, b, c, d)):
        out_ref[:, i * 128 : (i + 1) * 128] = ref[...]


def project_body(own_ref, other_ref, *refs):
    z, c, y = lax.axis_index("z"), lax.axis_index("c"), lax.axis_index("y")
    pieces, outs = refs[:-4], refs[-4:]
    tok = pieces[0].shape[0] // 4
    wide = own_ref.shape[1] // 4
    own, other = own_ref[...], other_ref[...]
    for s, out_ref in enumerate(outs):
        rows = pl.ds(pl.multiple_of(lax.rem(y + s, 4) * tok, tok), tok)
        heads = jnp.concatenate([piece[rows, :] for piece in pieces], axis=0)
        for weight, core in ((own, c), (other, 1 - c)):
            part = dot(heads, weight).astype(BF16)
            for t in range(4):
                at = pl.multiple_of((lax.rem(z + t, 4) * 2 + core) * wide, wide)
                out_ref[:, pl.ds(at, wide)] = part[:, t * wide : (t + 1) * wide]


def total_body(a, b, c, d, *outs):
    tok = outs[0].shape[0]
    for i, out_ref in enumerate(outs):
        rows = slice(i * tok, (i + 1) * tok)
        total = a[rows, :].astype(F32) + b[rows, :].astype(F32)
        total = total + c[rows, :].astype(F32) + d[rows, :].astype(F32)
        out_ref[...] = total.astype(out_ref.dtype)


def norm_body(p0, p1, p2, p3, residual_ref, gain_ref, hidden_ref, normed_ref):
    x = lax.axis_index("x")
    tok, model = residual_ref.shape
    width = model // 4
    square = jnp.zeros((tok, 1), F32)
    for s, piece in enumerate((p0, p1, p2, p3)):
        cols = pl.ds(pl.multiple_of(lax.rem(x + 4 - s, 4) * width, width), width)
        total = residual_ref[:, cols].astype(F32) + piece[...].astype(F32)
        hidden_ref[:, cols] = total
        square = square + jnp.sum(total * total, axis=-1, keepdims=True)
    scale = lax.rsqrt(square * (1.0 / model) + 1e-06)
    normed_ref[...] = (hidden_ref[...] * scale * gain_ref[...]).astype(BF16)


def routing(core, ids, slots):
    tokens = ids.shape[0]
    half = tokens // 2
    slot = lax.broadcasted_iota(jnp.int32, (tokens, slots), 1)
    token = lax.broadcasted_iota(jnp.int32, (tokens, slots), 0)
    chip = slot // (2 * SLOTS)
    expert = ((chip // 4) * 2 + core) * 4 + chip % 4
    named = [ids[:, j : j + 1] == expert for j in range(ids.shape[1])]
    match = named[0]
    for one in named[1:]:
        match = match | one
    r = lax.broadcasted_iota(jnp.int32, (tokens, tokens), 0)
    c = lax.broadcasted_iota(jnp.int32, (tokens, tokens), 1)
    ahead = (c < r) & ((c < half) == (r < half))
    rank = dot(ahead.astype(BF16), match.astype(BF16)).astype(jnp.int32)
    here = match & (rank == slot % SLOTS) & ((token < half) == (slot % (2 * SLOTS) < SLOTS))
    return here, named


def load_body(source, out_ref, sem):
    rows = out_ref.shape[0]
    copy = pltpu.make_async_copy(source.at[0, pl.ds(rows, rows), :], out_ref, sem)
    copy.start()
    copy.wait()


def expert_body(rows_ref, first_ref, second_ref, down_ref, out_ref, act_ref):
    tile, ff = act_ref.shape
    half = first_ref.shape[0]

    def step(m, carry):
        at = pl.ds(pl.multiple_of(m * tile, tile), tile)
        left, right = rows_ref[at, :half], rows_ref[at, half:]
        gate = dot(left, first_ref[:, :ff]) + dot(right, second_ref[:, :ff])
        up = dot(left, first_ref[:, ff:]) + dot(right, second_ref[:, ff:])
        act_ref[...] = (gate / (1.0 + jnp.exp(-gate)) * up).astype(BF16)
        out_ref[at, :] = dot(act_ref[...], down_ref[...]).astype(BF16)
        return carry

    lax.fori_loop(0, rows_ref.shape[0] // tile, step, 0)


def pack_body(ids_ref, gates_ref, out_ref):
    top = ids_ref.shape[0]
    out_ref[:top] = ids_ref[...].astype(F32)
    out_ref[top:] = gates_ref[...]


def tables_body(own_ref, sibling_ref, table_ref, weights_ref):
    tokens, slots = table_ref.shape
    top = own_ref.shape[0] // 2
    route = jnp.concatenate([own_ref[...].T, sibling_ref[...].T], axis=0)
    ids = route[:, :top].astype(jnp.int32)
    gates = route[:, top:]
    here, named = routing(lax.axis_index("c"), ids, slots)
    weight = jnp.zeros(here.shape, F32)
    for j, one in enumerate(named):
        weight = weight + jnp.where(one, gates[:, j : j + 1], 0.0)
    weight = jnp.where(here, weight, 0.0)
    high = weight.astype(BF16)
    table_ref[...] = here.astype(BF16)
    weights_ref[:tokens] = high
    weights_ref[tokens:] = (weight - high.astype(F32)).astype(BF16)


def dispatch_body(table_ref, own_ref, other_ref, out_ref):
    tokens = jnp.concatenate([own_ref[...], other_ref[...]], axis=0)
    out_ref[...] = dot(table_ref[...], tokens, ((0,), (0,))).astype(BF16)


def combine_body(results_ref, weights_ref, hidden_ref, own_ref, other_ref):
    total = dot(weights_ref[...], results_ref[...])
    tok = hidden_ref.shape[0]
    other_ref[...] = total[tok : 2 * tok] + total[3 * tok :]
    own_ref[...] = hidden_ref[...] + (total[:tok] + total[2 * tok : 3 * tok])


def finish_body(own_ref, other_ref, out_ref):
    out_ref[...] = (own_ref[...] + other_ref[...]).astype(BF16)


def layer(
    queries,
    keys,
    values,
    document_index,
    out_proj,
    residual_in,
    norm_gain,
    expert_ids,
    gate_weights,
    w_gate_up,
    w_down,
):
    tok, model = residual_in.shape
    tokens, head_cols = queries.shape
    ff = w_down.shape[1]
    slots = 64 * 2 * SLOTS
    width = model // 4

    columns = [ring(out_proj, "z", s, 4) for s in (1, 2, 3)]
    inputs = (queries, keys, values, document_index)
    half_rows = shape((model // 2, 2 * ff), BF16)
    heads, first = call(
        attention_body, [shape((tokens, head_cols), BF16), half_rows],
        *inputs, w_gate_up, flops=10**10, hbm=(*inputs, w_gate_up),
        scratch=[VMEM(a.shape, a.dtype) for a in inputs]
        + [pltpu.SemaphoreType.DMA((4,)), pltpu.SemaphoreType.DMA(())],
    )
    near = [heads] + [ring(heads, "x", s, 4) for s in (1, 3)]
    far = [ring(heads, "x", 2, 4)]
    second = call(
        load_body, half_rows, w_gate_up, hbm=(w_gate_up,), flops=10**9,
        scratch=[pltpu.SemaphoreType.DMA(())],
    )
    own_cols = call(
        join_body, shape((head_cols, model // 8), BF16),
        out_proj, *columns,
    )
    other_cols = ring(own_cols, "c", 1, 2)

    route = call(
        pack_body, shape((2 * expert_ids.shape[1], tok), F32),
        expert_ids.T, gate_weights.T,
    )
    sibling = ring(route, "c", 1, 2)
    table, weights = call(
        tables_body, [shape((2 * tok, slots), BF16), shape((4 * tok, slots), BF16)],
        route, sibling,
    )

    parts = {}
    for name, pieces in (("near", near), ("far", far)):
        outs = [shape((len(pieces) * tok, width), BF16)] * 4
        operands = (own_cols, other_cols, *pieces)
        mine, *sent = call(project_body, outs, *operands, flops=10**9)
        across = ring(sent[1], "y", -2, 4)
        got = [across, ring(sent[0], "y", -1, 4), ring(sent[2], "y", -3, 4)]
        kinds = [F32, BF16, BF16] if name == "near" else [BF16]
        sums = call(total_body, [shape((tok, width), k) for k in kinds], mine, *got)
        for s, v in zip((0, 1, 3) if name == "near" else (2,), sums):
            parts[s] = ring(v, "x", -s, 4) if s else v

    hidden, normed = call(
        norm_body, [shape((tok, model), F32), shape((tok, model), BF16)],
        *[parts[s] for s in range(4)], residual_in, norm_gain.reshape(1, model),
    )

    outgoing = call(
        dispatch_body, shape((slots, model), BF16),
        table, normed, ring(normed, "c", 1, 2),
    )
    rows = lax.all_to_all(
        outgoing.reshape(64, 2 * SLOTS, model), ("x", "z", "y"), 0, 0, tiled=True
    ).reshape(slots, model)

    expert_out = call(
        expert_body, shape((slots, model), BF16), rows, first, second, w_down[0],
        flops=10**10, scratch=[VMEM((256, ff), BF16)],
    )
    results = lax.all_to_all(
        expert_out.reshape(64, 2 * SLOTS, model), ("x", "z", "y"), 0, 0, tiled=True
    ).reshape(slots, model)
    own, other = call(combine_body, [shape((tok, model), F32)] * 2, results, weights, hidden)
    return call(finish_body, shape((tok, model), BF16), own, ring(other, "c", 1, 2), out=False)


def solution(mesh):
    fine = Mesh(mesh.devices.reshape(4, 4, 2, 4), ("x", "z", "c", "y"))
    group = ("x", "z", "c")
    every = group + ("y",)
    in_specs = (
        P(group, "y"),
        P(group, "y"),
        P(group, "y"),
        P(group, None),
        P("y", group),
        P(every, None),
        P(),
        P(every, None),
        P(every, None),
        P(every, None, None),
        P(every, None, None),
    )
    return jax.shard_map(
        layer, mesh=fine, in_specs=in_specs, out_specs=P(every, None), check_vma=False
    )
```
